32 devices in a mesh: freq: 32 (over z, y, x, core).
Axes of the slice: x: 2, y: 2, z: 4, core: 2. Of those that a mesh axis runs over, the one named last changes fastest.
Arguments:
- pulses: float32 [1, 2, 30, 65536], P(None, None, None, 'freq'), may hold values from -4 to 4
- coupling: float32 [2, 30, 30, 65536], P(None, None, None, 'freq'), may hold values from -0.4 to 0.4
- dispersion_terms: float32 [3, 30], replicated, may hold values from -3 to 3
- kerr_gain: float32 [30], replicated, may hold values from 0.01 to 0.08
Outputs:
- evolved: float32 [1, 2, 30, 65536], P(None, None, None, 'freq')
The draws below stay inside these ranges and needn't reach their ends.
All inputs are finite; a program needn't handle non-finite values.
Results may differ from the reference program's by a relative error of at most 0.00027.
Values sent between devices are 32-bit elements; how exact they have to be, the bound alone decides.
A program may use at most 128 MiB of HBM per device.

```python
import math
import jax
import jax.numpy as jnp
from jax import lax

M = 30
TPTS = 65536
STEPS = 2
PULSES = 1
FLOC = 2048
N_FREQ = 32


def steps_of(key, shape, cuts, smallest, top_value):
    def one(dim, shards_of):
        draws = jax.random.uniform(jax.random.fold_in(jax.random.fold_in(key, 6), dim), (shards_of,), jnp.float32, smallest / len(cuts), top_value / len(cuts))
        return jnp.repeat(jnp.exp(draws), shape[dim] // shards_of).reshape((-1,) + (1,) * (len(shape) - dim - 1))

    gain = one(*cuts[0])
    for cut in cuts[1:]:
        gain = gain * one(*cut)
    return gain


def noise(key, shape, spread, bound, split=(), kind=jnp.bfloat16):
    gain = steps_of(key, shape, split, -0.22, 0.18) if split else 1.0
    entries = jax.random.normal(key, shape, jnp.float32) * spread * gain
    return jnp.minimum(jnp.maximum(entries, -bound), bound).astype(kind)


def setup_inputs(seed: int = 0) -> dict:
    key_list = jax.random.split(jax.random.key(seed), 5)
    return {
        "pulses": noise(key_list[0], (PULSES, 2, M, TPTS), 0.5, 4.0, ((3, 32),), jnp.float32),
        "coupling": noise(key_list[1], (2, M, M, TPTS), 0.06, 0.4, ((3, 32),), jnp.float32),
        "dispersion_terms": jnp.clip(jax.random.uniform(key_list[2], (3, M), jnp.float32, -3.0, 3.0), -3.0, 3.0),
        "kerr_gain": jnp.clip(jnp.exp(jax.random.uniform(key_list[3], (M,), jnp.float32, math.log(0.01), math.log(0.08))), 0.01, 0.08),
    }


def reference(pulses, coupling, dispersion_terms, kerr_gain):
    complex_field = pulses[:, 0] + 1j * pulses[:, 1]
    bin_order = coupling.reshape(2, M, M, N_FREQ, FLOC).transpose(0, 1, 2, 4, 3).reshape(2, M, M, TPTS)
    identity = jnp.eye(M, dtype=jnp.float32)[:, :, None]
    mixing = (bin_order[0] + identity) + 1j * bin_order[1]
    bin_index = jnp.arange(TPTS, dtype=jnp.int32)
    signed_bin = jnp.where(bin_index < TPTS // 2, bin_index, bin_index - TPTS).astype(jnp.float32)
    angular = signed_bin / (TPTS // 2)
    dispersion = (dispersion_terms[0][:, None] * angular + dispersion_terms[1][:, None] * angular ** 2 / 2
                  + dispersion_terms[2][:, None] * angular ** 3 / 6)
    rotation = jnp.cos(dispersion) + 1j * jnp.sin(dispersion)
    for repeat in range(STEPS):
        spectrum = jnp.fft.fft(complex_field, axis=-1)
        spectrum = jnp.einsum("nmk,bmk->bnk", mixing, spectrum, precision=lax.Precision.HIGHEST)
        spectrum = spectrum * rotation
        complex_field = jnp.fft.ifft(spectrum, axis=-1)
        magnitude = jnp.real(complex_field) ** 2 + jnp.imag(complex_field) ** 2
        total_power = jnp.sum(magnitude, axis=1, keepdims=True)
        nonlinear = kerr_gain[None, :, None] * (2.0 * total_power - magnitude)
        complex_field = complex_field * (jnp.cos(nonlinear) + 1j * jnp.sin(nonlinear))
    return jnp.stack((jnp.real(complex_field), jnp.imag(complex_field)), axis=1).astype(jnp.float32)
```

```python
import functools

import jax
import jax.numpy as jnp
import numpy as np
from jax import lax
from jax.experimental import pallas as pl
from jax.experimental.pallas import tpu as pltpu
from jax.sharding import PartitionSpec as P

STEPS = 2


HIGHEST = lax.Precision.HIGHEST


def angle_table(first, second, modulus, orient):
    turns = first[:, None] * second[None, :] % modulus
    radians = turns.astype(jnp.float32) * (2.0 * jnp.pi / modulus)
    return (jnp.cos(radians), orient * jnp.sin(radians))


def rotate(real_part, imag_part, cosine, sine):
    return (real_part * cosine - imag_part * sine, real_part * sine + imag_part * cosine)


def transform(stacked, cosine, sine):
    real_part = stacked[:, 0]
    imag_part = stacked[:, 1]
    out_real = jnp.matmul(real_part, cosine, precision=HIGHEST) - jnp.matmul(
        imag_part, sine, precision=HIGHEST
    )
    out_imag = jnp.matmul(real_part, sine, precision=HIGHEST) + jnp.matmul(
        imag_part, cosine, precision=HIGHEST
    )
    return jnp.stack((out_real, out_imag), axis=1)


def nonlinear_phase(stacked, kerr_gain):
    magnitude = stacked[:, 0] ** 2 + stacked[:, 1] ** 2
    total_power = jnp.sum(magnitude, axis=1, keepdims=True)
    gains = kerr_gain.reshape((1, -1) + (1,) * (magnitude.ndim - 2))
    angles = gains * (2.0 * total_power - magnitude)
    real_part, imag_part = rotate(stacked[:, 0], stacked[:, 1], jnp.cos(angles), jnp.sin(angles))
    return jnp.stack((real_part, imag_part), axis=1)


def per_device(pulses, coupling, dispersion_terms, kerr_gain):
    shards = lax.axis_size("freq")
    device = lax.axis_index("freq")
    mode_count = pulses.shape[2]
    local_count = pulses.shape[3]
    groups = local_count // shards
    total_count = local_count * shards
    column_index = jnp.arange(shards, dtype=jnp.int32)
    row_index = jnp.arange(local_count, dtype=jnp.int32)
    short_cos, short_sin = angle_table(column_index, column_index, shards, -1.0)
    inverse_short_cos, inverse_short_sin = angle_table(column_index, column_index, shards, 1.0)
    long_cos, long_sin = angle_table(row_index, row_index, local_count, -1.0)
    inverse_long_cos, inverse_long_sin = angle_table(row_index, row_index, local_count, 1.0)
    sample_rows = jnp.arange(groups, dtype=jnp.int32) * shards + device
    twist_cos, twist_sin = angle_table(sample_rows, column_index, total_count, -1.0)
    untwist_cos, untwist_sin = angle_table(row_index, jnp.reshape(device, (1,)), total_count, 1.0)
    untwist_cos = untwist_cos.reshape(-1)
    untwist_sin = untwist_sin.reshape(-1)
    bins = device + shards * row_index
    signed_bin = jnp.where(bins < total_count // 2, bins, bins - total_count).astype(jnp.float32)
    angular = signed_bin / (total_count // 2)
    dispersion = (
        dispersion_terms[0][:, None] * angular
        + dispersion_terms[1][:, None] * angular**2 / 2
        + dispersion_terms[2][:, None] * angular**3 / 6
    )
    spread_cos = jnp.cos(dispersion)
    spread_sin = jnp.sin(dispersion)
    identity = jnp.eye(mode_count, dtype=jnp.float32)[:, :, None]
    mixing_real = coupling[0] + identity
    mixing_imag = coupling[1]
    blocks = pulses.reshape(pulses.shape[0], 2, mode_count, groups, shards)
    columns = lax.all_to_all(blocks, "freq", split_axis=4, concat_axis=4, tiled=True)
    for repeat in range(STEPS):
        spectral = transform(columns, short_cos, short_sin)
        forward_real_part, forward_imag_part = rotate(
            spectral[:, 0], spectral[:, 1], twist_cos, twist_sin
        )
        evolve_rows = lax.all_to_all(
            jnp.stack((forward_real_part, forward_imag_part), axis=1),
            "freq",
            split_axis=4,
            concat_axis=4,
            tiled=True,
        )
        flat = evolve_rows.reshape(evolve_rows.shape[0], 2, mode_count, local_count)
        spectrum = transform(flat, long_cos, long_sin)
        spec_real = spectrum[:, 0]
        spec_imag = spectrum[:, 1]
        mixed_real = jnp.einsum(
            "nmk,bmk->bnk", mixing_real, spec_real, precision=HIGHEST
        ) - jnp.einsum("nmk,bmk->bnk", mixing_imag, spec_imag, precision=HIGHEST)
        mixed_imag = jnp.einsum(
            "nmk,bmk->bnk", mixing_real, spec_imag, precision=HIGHEST
        ) + jnp.einsum("nmk,bmk->bnk", mixing_imag, spec_real, precision=HIGHEST)
        real_part, imag_part = rotate(mixed_real, mixed_imag, spread_cos, spread_sin)
        inverted = transform(
            jnp.stack((real_part, imag_part), axis=1), inverse_long_cos, inverse_long_sin
        )
        real_part, imag_part = rotate(inverted[:, 0], inverted[:, 1], untwist_cos, untwist_sin)
        moved = jnp.stack((real_part, imag_part), axis=1).reshape(evolve_rows.shape)
        columns = nonlinear_phase(
            transform(
                lax.all_to_all(moved, "freq", split_axis=4, concat_axis=4, tiled=True),
                inverse_short_cos,
                inverse_short_sin,
            )
            * (1.0 / total_count),
            kerr_gain,
        )
    returned = lax.all_to_all(columns, "freq", split_axis=4, concat_axis=4, tiled=True)
    return returned.reshape(columns.shape[0], 2, mode_count, local_count)


LANES = 128
HALF = LANES // 2
SUB = 8


def low_lanes(shape):
    return lax.broadcasted_iota(jnp.int32, shape, len(shape) - 1) < HALF


def swap(x):
    return pltpu.roll(x, HALF, 1)


def sign_row(rows):
    return jnp.where(low_lanes((rows, LANES)), -1.0, 1.0).astype(jnp.float32)


def times_root(x, index, count, orient, sgn):
    eighth = 8 * index
    if index == 0:
        return x
    if eighth == 2 * count:
        return swap(x) * (sgn * orient)
    angle = 2.0 * np.pi * index / count
    return x * float(np.cos(angle)) + swap(x) * (sgn * float(orient * np.sin(angle)))


def short_fft(items, orient, sgn):
    count = len(items)
    if count == 1:
        return items
    even = short_fft(items[0::2], orient, sgn)
    odd = short_fft(items[1::2], orient, sgn)
    turned = [times_root(v, k, count, orient, sgn) for k, v in enumerate(odd)]
    return [e + t for e, t in zip(even, turned)] + [e - t for e, t in zip(even, turned)]


def packed_mul(x, cosine, signed_sine):
    return x * cosine + swap(x) * signed_sine


def split_constant(value, pieces, bits):
    parts = []
    for _ in range(pieces - 1):
        exponent = np.floor(np.log2(value))
        unit = 2.0 ** (exponent - bits + 1)
        part = np.floor(value / unit) * unit
        parts.append(float(part))
        value -= part
    return parts + [float(value)]


HALF_PI = split_constant(np.pi / 2, 4, 8)


def sine_cosine(theta):
    turns = jnp.floor(theta * float(2 / np.pi) + 0.5)
    rest = theta
    for part in HALF_PI:
        rest = rest - turns * part
    square = rest * rest
    sine = rest + rest * square * (
        -1.6666654611e-1 + square * (8.3321608736e-3 - square * 1.9515295891e-4)
    )
    cosine = 1.0 - 0.5 * square + square * square * (
        4.166664568298827e-2 + square * (-1.388731625493765e-3 + square * 2.443315711809948e-5)
    )
    quadrant = turns.astype(jnp.int32) & 3
    crossed = (quadrant & 1) == 1
    out_sine = jnp.where(crossed, cosine, sine)
    out_cosine = jnp.where(crossed, sine, cosine)
    out_sine = jnp.where(quadrant >= 2, -out_sine, out_sine)
    out_cosine = jnp.where((quadrant == 1) | (quadrant == 2), -out_cosine, out_cosine)
    return out_sine, out_cosine


def exchange_kernel(count, x_ref, out_ref, send_sem, recv_sem, local_sem):
    me = lax.axis_index("freq")
    barrier = pltpu.get_barrier_semaphore()

    def greet(k, carry):
        pl.semaphore_signal(
            barrier, inc=1, device_id=((me + k) % count,), device_id_type=pl.DeviceIdType.MESH
        )
        return carry

    lax.fori_loop(1, count, greet, 0)
    own = pltpu.make_async_copy(x_ref.at[me], out_ref.at[me], local_sem)
    own.start()
    pl.semaphore_wait(barrier, count - 1)

    def copy(k, slot):
        peer = (me + k) % count
        return pltpu.make_async_remote_copy(
            src_ref=x_ref.at[peer],
            dst_ref=out_ref.at[slot],
            send_sem=send_sem.at[k],
            recv_sem=recv_sem.at[k],
            device_id=(peer,),
            device_id_type=pl.DeviceIdType.MESH,
        )

    def send(k, carry):
        copy(k, me).start()
        return carry

    def drain(k, carry):
        copy(k, (me - k + count) % count).wait_recv()
        return carry

    def finish(k, carry):
        copy(k, me).wait_send()
        return carry

    lax.fori_loop(1, count, send, 0)
    own.wait()
    lax.fori_loop(1, count, drain, 0)
    lax.fori_loop(1, count, finish, 0)


def exchange(x):
    count = x.shape[0]
    return pl.pallas_call(
        functools.partial(exchange_kernel, count),
        out_shape=jax.ShapeDtypeStruct(x.shape, x.dtype),
        in_specs=[pl.BlockSpec(memory_space=pltpu.VMEM)],
        out_specs=pl.BlockSpec(memory_space=pltpu.VMEM),
        scratch_shapes=[
            pltpu.SemaphoreType.DMA((count,)),
            pltpu.SemaphoreType.DMA((count,)),
            pltpu.SemaphoreType.DMA(()),
        ],
        compiler_params=pltpu.CompilerParams(collective_id=0, has_side_effects=True),
        name="exchange",
    )(x)


def column_kernel(inverse, forward, scale, x_ref, cos_ref, sin_ref, gain_ref, out_ref, field):
    count, rows = x_ref.shape[0], x_ref.shape[1]
    sgn = sign_row(SUB)

    def chunk(c):
        return pl.ds(pl.multiple_of(c * SUB, SUB), SUB)

    if inverse:

        def undo(c, carry):
            rows_of = chunk(c)
            items = [
                packed_mul(
                    x_ref[d, rows_of, :], cos_ref[d : d + 1, :] * scale, sin_ref[d : d + 1, :] * -scale
                )
                for d in range(count)
            ]
            for a, value in enumerate(short_fft(items, 1.0, sgn)):
                field[a, rows_of, :] = value
            return carry

        lax.fori_loop(0, rows // SUB, undo, 0)
        wide = sign_row(rows)
        target = field if forward else out_ref

        def kerr(a, carry):
            x = field[a]
            square = x * x
            magnitude = square + swap(square)
            power = jnp.sum(magnitude, axis=0, keepdims=True)
            sine, cosine = sine_cosine(gain_ref[...] * (2.0 * power - magnitude))
            target[a] = packed_mul(x, cosine, sine * wide)
            return carry

        lax.fori_loop(0, count, kerr, 0, unroll=2)
    if forward:
        source = field if inverse else x_ref

        def apply(c, carry):
            rows_of = chunk(c)
            items = short_fft([source[a, rows_of, :] for a in range(count)], -1.0, sgn)
            for d, value in enumerate(items):
                out_ref[d, rows_of, :] = packed_mul(value, cos_ref[d : d + 1, :], sin_ref[d : d + 1, :])
            return carry

        lax.fori_loop(0, rows // SUB, apply, 0)


def column_stage(x, twist_cos, twist_sin, gain, scale, inverse, forward):
    return pl.pallas_call(
        functools.partial(column_kernel, inverse, forward, scale),
        out_shape=jax.ShapeDtypeStruct(x.shape, x.dtype),
        in_specs=[pl.BlockSpec(memory_space=pltpu.VMEM)] * 4,
        out_specs=pl.BlockSpec(memory_space=pltpu.VMEM),
        scratch_shapes=[pltpu.VMEM(x.shape, jnp.float32)],
        name="column",
    )(x, twist_cos, twist_sin, gain)


def long_dft(x, weights):
    high = x.astype(jnp.bfloat16)
    low = (x - high.astype(jnp.float32)).astype(jnp.bfloat16)
    both = jnp.concatenate((high, low), axis=1)
    product = jnp.dot(both, weights, preferred_element_type=jnp.float32)
    return product[:, :LANES] + product[:, LANES:]


def row_kernel(
    x_ref, c_ref, spread_cos_ref, spread_sin_ref, tw_cos_ref, tw_sin_ref, fwd_ref, inv_ref,
    out_ref, spec, mixed, sum_real, sum_imag,
):
    tile = pl.program_id(0)
    count, rows = x_ref.shape[0], x_ref.shape[1]
    modes = c_ref.shape[1]
    sgn = sign_row(SUB)

    def chunk(c):
        return pl.ds(pl.multiple_of(c * SUB, SUB), SUB)

    @pl.when(tile == 0)
    def _():
        sum_real[...] = jnp.zeros_like(sum_real)
        sum_imag[...] = jnp.zeros_like(sum_imag)

        def lanes(q, carry):
            part = pl.ds(q * 4, 4)
            block = x_ref[part].reshape(4 * rows, LANES)
            spec[part] = long_dft(block, fwd_ref[...]).reshape(4, rows, LANES)
            return carry

        lax.fori_loop(0, count // 4, lanes, 0)

        def across(c, carry):
            rows_of = chunk(c)
            items = [
                packed_mul(spec[p, rows_of, :], tw_cos_ref[p : p + 1, :], tw_sin_ref[p : p + 1, :])
                for p in range(count)
            ]
            for j, value in enumerate(short_fft(items, -1.0, sgn)):
                spec[j, rows_of, :] = value
            return carry

        lax.fori_loop(0, rows // SUB, across, 0)

    first, second = spec[2 * tile], spec[2 * tile + 1]
    low = low_lanes((rows, LANES))
    real = jnp.where(low, first, swap(second))
    imag = jnp.where(low, swap(first), second)
    real_part, imag_part = real[:modes], imag[:modes]
    for n in range(modes):
        coup_real, coup_imag = c_ref[0, n], c_ref[1, n]
        sum_real[n : n + 1, :] = jnp.sum(
            coup_real * real_part - coup_imag * imag_part, axis=0, keepdims=True
        )
        sum_imag[n : n + 1, :] = jnp.sum(
            coup_real * imag_part + coup_imag * real_part, axis=0, keepdims=True
        )
    total_real, total_imag = sum_real[...] + real, sum_imag[...] + imag
    total_real, total_imag = rotate(
        total_real, total_imag, spread_cos_ref[...], spread_sin_ref[...]
    )
    mixed[2 * tile] = jnp.where(low, total_real, swap(total_imag))
    mixed[2 * tile + 1] = jnp.where(low, swap(total_real), total_imag)

    @pl.when(tile == pl.num_programs(0) - 1)
    def _():
        def across(c, carry):
            rows_of = chunk(c)
            items = short_fft([mixed[j, rows_of, :] for j in range(count)], 1.0, sgn)
            for p, value in enumerate(items):
                mixed[p, rows_of, :] = packed_mul(
                    value, tw_cos_ref[p : p + 1, :], -tw_sin_ref[p : p + 1, :]
                )
            return carry

        lax.fori_loop(0, rows // SUB, across, 0)

        def lanes(q, carry):
            part = pl.ds(q * 4, 4)
            block = mixed[part].reshape(4 * rows, LANES)
            out_ref[part] = long_dft(block, inv_ref[...]).reshape(4, rows, LANES)
            return carry

        lax.fori_loop(0, count // 4, lanes, 0)


def row_stage(x, coupling, spread_cos, spread_sin, tw_cos, tw_sin, fwd, inv):
    rows = x.shape[1]
    modes = coupling.shape[1]
    tiles = coupling.shape[3] // LANES
    whole = lambda array: pl.BlockSpec(array.shape, lambda t: (0,) * array.ndim)
    return pl.pallas_call(
        row_kernel,
        grid=(tiles,),
        out_shape=jax.ShapeDtypeStruct(x.shape, x.dtype),
        in_specs=[
            whole(x),
            pl.BlockSpec((2, modes, modes, LANES), lambda t: (0, 0, 0, t)),
            pl.BlockSpec((rows, LANES), lambda t: (0, t)),
            pl.BlockSpec((rows, LANES), lambda t: (0, t)),
            whole(tw_cos),
            whole(tw_sin),
            whole(fwd),
            whole(inv),
        ],
        out_specs=whole(x),
        scratch_shapes=[
            pltpu.VMEM(x.shape, jnp.float32),
            pltpu.VMEM(x.shape, jnp.float32),
            pltpu.VMEM((rows, LANES), jnp.float32),
            pltpu.VMEM((rows, LANES), jnp.float32),
        ],
        compiler_params=pltpu.CompilerParams(dimension_semantics=("arbitrary",)),
        name="row",
    )(x, coupling, spread_cos, spread_sin, tw_cos, tw_sin, fwd, inv)


def packed_table(cosine, sine):
    xp = np if isinstance(cosine, np.ndarray) else jnp
    return (
        xp.concatenate((cosine, cosine), axis=1).astype(xp.float32),
        xp.concatenate((-sine, sine), axis=1).astype(xp.float32),
    )


def dft_weights(size, orient):
    index = np.arange(size)
    angle = orient * 2.0 * np.pi * (index[:, None] * index[None, :] % size) / size
    cosine, sine = np.cos(angle), np.sin(angle)
    full = np.block([[cosine, sine], [-sine, cosine]]).astype(np.float32)
    high = full.astype(jnp.bfloat16)
    low = (full - high.astype(np.float32)).astype(jnp.bfloat16)
    return np.block([[high, low], [high, np.zeros_like(low)]])


def packed_device(pulses, coupling, dispersion_terms, kerr_gain):
    shards = lax.axis_size("freq")
    device = lax.axis_index("freq")
    modes, local = pulses.shape[2], pulses.shape[3]
    groups = local // shards
    total = local * shards
    rows = -(-modes // SUB) * SUB
    pad = rows - modes

    shard_index = np.arange(shards)
    angle = -2.0 * np.pi * (shard_index[:, None] * np.arange(groups)[None, :] % local) / local
    tw_cos, tw_sin = packed_table(np.cos(angle), np.sin(angle))
    fwd, inv = dft_weights(groups, -1.0), dft_weights(groups, 1.0)
    samples = device + shards * jnp.arange(groups, dtype=jnp.int32)
    twist_cos, twist_sin = packed_table(
        *angle_table(jnp.arange(shards, dtype=jnp.int32), samples, total, -1.0)
    )
    gain = jnp.broadcast_to(jnp.pad(kerr_gain, (0, pad))[:, None], (rows, LANES))

    bins = device + shards * jnp.arange(local, dtype=jnp.int32)
    signed_bin = jnp.where(bins < total // 2, bins, bins - total).astype(jnp.float32)
    angular = signed_bin / (total // 2)
    terms = jnp.pad(dispersion_terms, ((0, 0), (0, pad)))
    dispersion = (
        terms[0][:, None] * angular
        + terms[1][:, None] * angular**2 / 2
        + terms[2][:, None] * angular**3 / 6
    )
    spread_cos, spread_sin = jnp.cos(dispersion), jnp.sin(dispersion)

    blocks = pulses.reshape(2, modes, groups, shards).transpose(3, 1, 0, 2)
    x = jnp.pad(blocks.reshape(shards, modes, 2 * groups), ((0, 0), (0, pad), (0, 0)))
    scale = 1.0 / total
    for repeat in range(STEPS):
        x = exchange(x) if repeat == 0 else x
        if repeat == 0:
            x = column_stage(x, twist_cos, twist_sin, gain, scale, False, True)
        x = exchange(x)
        x = row_stage(x, coupling, spread_cos, spread_sin, tw_cos, tw_sin, fwd, inv)
        x = exchange(x)
        x = column_stage(x, twist_cos, twist_sin, gain, scale, True, repeat < STEPS - 1)
    x = exchange(x)
    x = x[:, :modes].reshape(shards, modes, 2, groups).transpose(2, 1, 3, 0)
    return x.reshape(1, 2, modes, local)


def fits(shards, pulses):
    local = pulses.shape[3] // shards
    return (
        pulses.shape[0] == 1
        and shards & (shards - 1) == 0
        and shards >= 4
        and local == shards * HALF
    )


def solution(mesh):
    in_specs = (P(None, None, None, "freq"), P(None, None, None, "freq"), P(), P())
    out_specs = P(None, None, None, "freq")
    shards = mesh.shape["freq"]

    def run(pulses, coupling, dispersion_terms, kerr_gain):
        body = packed_device if fits(shards, pulses) else per_device
        return jax.shard_map(
            body, mesh=mesh, in_specs=in_specs, out_specs=out_specs, check_vma=False
        )(pulses, coupling, dispersion_terms, kerr_gain)

    return run
```

```python
import functools

import jax
import jax.numpy as jnp
import numpy as np
from jax import lax
from jax.experimental import pallas as pl
from jax.experimental.pallas import tpu as pltpu
from jax.sharding import PartitionSpec as P

STEPS = 2


HIGHEST = lax.Precision.HIGHEST


def angle_table(first, second, modulus, orient):
    turns = first[:, None] * second[None, :] % modulus
    radians = turns.astype(jnp.float32) * (2.0 * jnp.pi / modulus)
    return (jnp.cos(radians), orient * jnp.sin(radians))


def rotate(real_part, imag_part, cosine, sine):
    return (real_part * cosine - imag_part * sine, real_part * sine + imag_part * cosine)


def transform(stacked, cosine, sine):
    real_part = stacked[:, 0]
    imag_part = stacked[:, 1]
    out_real = jnp.matmul(real_part, cosine, precision=HIGHEST) - jnp.matmul(
        imag_part, sine, precision=HIGHEST
    )
    out_imag = jnp.matmul(real_part, sine, precision=HIGHEST) + jnp.matmul(
        imag_part, cosine, precision=HIGHEST
    )
    return jnp.stack((out_real, out_imag), axis=1)


def nonlinear_phase(stacked, kerr_gain):
    magnitude = stacked[:, 0] ** 2 + stacked[:, 1] ** 2
    total_power = jnp.sum(magnitude, axis=1, keepdims=True)
    gains = kerr_gain.reshape((1, -1) + (1,) * (magnitude.ndim - 2))
    angles = gains * (2.0 * total_power - magnitude)
    real_part, imag_part = rotate(stacked[:, 0], stacked[:, 1], jnp.cos(angles), jnp.sin(angles))
    return jnp.stack((real_part, imag_part), axis=1)


def per_device(pulses, coupling, dispersion_terms, kerr_gain):
    shards = lax.axis_size("freq")
    device = lax.axis_index("freq")
    mode_count = pulses.shape[2]
    local_count = pulses.shape[3]
    groups = local_count // shards
    total_count = local_count * shards
    column_index = jnp.arange(shards, dtype=jnp.int32)
    row_index = jnp.arange(local_count, dtype=jnp.int32)
    short_cos, short_sin = angle_table(column_index, column_index, shards, -1.0)
    inverse_short_cos, inverse_short_sin = angle_table(column_index, column_index, shards, 1.0)
    long_cos, long_sin = angle_table(row_index, row_index, local_count, -1.0)
    inverse_long_cos, inverse_long_sin = angle_table(row_index, row_index, local_count, 1.0)
    sample_rows = jnp.arange(groups, dtype=jnp.int32) * shards + device
    twist_cos, twist_sin = angle_table(sample_rows, column_index, total_count, -1.0)
    untwist_cos, untwist_sin = angle_table(row_index, jnp.reshape(device, (1,)), total_count, 1.0)
    untwist_cos = untwist_cos.reshape(-1)
    untwist_sin = untwist_sin.reshape(-1)
    bins = device + shards * row_index
    signed_bin = jnp.where(bins < total_count // 2, bins, bins - total_count).astype(jnp.float32)
    angular = signed_bin / (total_count // 2)
    dispersion = (
        dispersion_terms[0][:, None] * angular
        + dispersion_terms[1][:, None] * angular**2 / 2
        + dispersion_terms[2][:, None] * angular**3 / 6
    )
    spread_cos = jnp.cos(dispersion)
    spread_sin = jnp.sin(dispersion)
    identity = jnp.eye(mode_count, dtype=jnp.float32)[:, :, None]
    mixing_real = coupling[0] + identity
    mixing_imag = coupling[1]
    blocks = pulses.reshape(pulses.shape[0], 2, mode_count, groups, shards)
    columns = lax.all_to_all(blocks, "freq", split_axis=4, concat_axis=4, tiled=True)
    for repeat in range(STEPS):
        spectral = transform(columns, short_cos, short_sin)
        forward_real_part, forward_imag_part = rotate(
            spectral[:, 0], spectral[:, 1], twist_cos, twist_sin
        )
        evolve_rows = lax.all_to_all(
            jnp.stack((forward_real_part, forward_imag_part), axis=1),
            "freq",
            split_axis=4,
            concat_axis=4,
            tiled=True,
        )
        flat = evolve_rows.reshape(evolve_rows.shape[0], 2, mode_count, local_count)
        spectrum = transform(flat, long_cos, long_sin)
        spec_real = spectrum[:, 0]
        spec_imag = spectrum[:, 1]
        mixed_real = jnp.einsum(
            "nmk,bmk->bnk", mixing_real, spec_real, precision=HIGHEST
        ) - jnp.einsum("nmk,bmk->bnk", mixing_imag, spec_imag, precision=HIGHEST)
        mixed_imag = jnp.einsum(
            "nmk,bmk->bnk", mixing_real, spec_imag, precision=HIGHEST
        ) + jnp.einsum("nmk,bmk->bnk", mixing_imag, spec_real, precision=HIGHEST)
        real_part, imag_part = rotate(mixed_real, mixed_imag, spread_cos, spread_sin)
        inverted = transform(
            jnp.stack((real_part, imag_part), axis=1), inverse_long_cos, inverse_long_sin
        )
        real_part, imag_part = rotate(inverted[:, 0], inverted[:, 1], untwist_cos, untwist_sin)
        moved = jnp.stack((real_part, imag_part), axis=1).reshape(evolve_rows.shape)
        columns = nonlinear_phase(
            transform(
                lax.all_to_all(moved, "freq", split_axis=4, concat_axis=4, tiled=True),
                inverse_short_cos,
                inverse_short_sin,
            )
            * (1.0 / total_count),
            kerr_gain,
        )
    returned = lax.all_to_all(columns, "freq", split_axis=4, concat_axis=4, tiled=True)
    return returned.reshape(columns.shape[0], 2, mode_count, local_count)


LANES = 128
HALF = LANES // 2
SUB = 8


def low_lanes(shape):
    return lax.broadcasted_iota(jnp.int32, shape, len(shape) - 1) < HALF


def swap(x):
    return pltpu.roll(x, HALF, 1)


def sign_row(rows):
    return jnp.where(low_lanes((rows, LANES)), -1.0, 1.0).astype(jnp.float32)


def times_root(x, index, count, orient, sgn):
    eighth = 8 * index
    if index == 0:
        return x
    if eighth == 2 * count:
        return swap(x) * (sgn * orient)
    angle = 2.0 * np.pi * index / count
    return x * float(np.cos(angle)) + swap(x) * (sgn * float(orient * np.sin(angle)))


def short_fft(items, orient, sgn):
    count = len(items)
    if count == 1:
        return items
    even = short_fft(items[0::2], orient, sgn)
    odd = short_fft(items[1::2], orient, sgn)
    turned = [times_root(v, k, count, orient, sgn) for k, v in enumerate(odd)]
    return [e + t for e, t in zip(even, turned)] + [e - t for e, t in zip(even, turned)]


def packed_mul(x, cosine, signed_sine):
    return x * cosine + swap(x) * signed_sine


def split_constant(value, pieces, bits):
    parts = []
    for _ in range(pieces - 1):
        exponent = np.floor(np.log2(value))
        unit = 2.0 ** (exponent - bits + 1)
        part = np.floor(value / unit) * unit
        parts.append(float(part))
        value -= part
    return parts + [float(value)]


HALF_PI = split_constant(np.pi / 2, 4, 8)


def sine_cosine(theta):
    turns = jnp.floor(theta * float(2 / np.pi) + 0.5)
    rest = theta
    for part in HALF_PI:
        rest = rest - turns * part
    square = rest * rest
    sine = rest + rest * square * (
        -1.6666654611e-1 + square * (8.3321608736e-3 - square * 1.9515295891e-4)
    )
    cosine = 1.0 - 0.5 * square + square * square * (
        4.166664568298827e-2 + square * (-1.388731625493765e-3 + square * 2.443315711809948e-5)
    )
    quadrant = turns.astype(jnp.int32) & 3
    crossed = (quadrant & 1) == 1
    out_sine = jnp.where(crossed, cosine, sine)
    out_cosine = jnp.where(crossed, sine, cosine)
    out_sine = jnp.where(quadrant >= 2, -out_sine, out_sine)
    out_cosine = jnp.where((quadrant == 1) | (quadrant == 2), -out_cosine, out_cosine)
    return out_sine, out_cosine


def exchange_kernel(count, modes, x_ref, out_ref, send_sem, recv_sem, local_sem):
    me = lax.axis_index("freq")
    barrier = pltpu.get_barrier_semaphore()
    rows = x_ref.shape[1]
    if rows > modes:
        spare = pl.ds(rows - SUB, SUB)
        out_ref[:, spare, :] = jnp.zeros((count, SUB, x_ref.shape[2]), x_ref.dtype)

    def greet(k, carry):
        pl.semaphore_signal(
            barrier, inc=1, device_id=((me + k) % count,), device_id_type=pl.DeviceIdType.MESH
        )
        return carry

    lax.fori_loop(1, count, greet, 0)
    own = pltpu.make_async_copy(
        x_ref.at[me, pl.ds(0, modes)], out_ref.at[me, pl.ds(0, modes)], local_sem
    )
    own.start()
    pl.semaphore_wait(barrier, count - 1)

    def copy(k, slot):
        peer = (me + k) % count
        return pltpu.make_async_remote_copy(
            src_ref=x_ref.at[peer, pl.ds(0, modes)],
            dst_ref=out_ref.at[slot, pl.ds(0, modes)],
            send_sem=send_sem.at[k],
            recv_sem=recv_sem.at[k],
            device_id=(peer,),
            device_id_type=pl.DeviceIdType.MESH,
        )

    def send(j, carry):
        copy(count // 2 + (j // 2) * (1 - 2 * (j % 2)), me).start()
        return carry

    def drain(k, carry):
        copy(k, (me - k + count) % count).wait_recv()
        return carry

    def finish(k, carry):
        copy(k, me).wait_send()
        return carry

    lax.fori_loop(1, count, send, 0)
    own.wait()
    lax.fori_loop(1, count, drain, 0)
    lax.fori_loop(1, count, finish, 0)


def exchange(x, modes):
    count = x.shape[0]
    return pl.pallas_call(
        functools.partial(exchange_kernel, count, modes),
        out_shape=jax.ShapeDtypeStruct(x.shape, x.dtype),
        in_specs=[pl.BlockSpec(memory_space=pltpu.VMEM)],
        out_specs=pl.BlockSpec(memory_space=pltpu.VMEM),
        scratch_shapes=[
            pltpu.SemaphoreType.DMA((count,)),
            pltpu.SemaphoreType.DMA((count,)),
            pltpu.SemaphoreType.DMA(()),
        ],
        compiler_params=pltpu.CompilerParams(collective_id=0, has_side_effects=True),
        name="exchange",
    )(x)


def column_kernel(inverse, forward, scale, x_ref, cos_ref, sin_ref, gain_ref, out_ref, field):
    count, rows = x_ref.shape[0], x_ref.shape[1]
    sgn = sign_row(SUB)

    def chunk(c):
        return pl.ds(pl.multiple_of(c * SUB, SUB), SUB)

    if inverse:

        def undo(c, carry):
            rows_of = chunk(c)
            items = [
                packed_mul(
                    x_ref[d, rows_of, :], cos_ref[d : d + 1, :] * scale, sin_ref[d : d + 1, :] * -scale
                )
                for d in range(count)
            ]
            for a, value in enumerate(short_fft(items, 1.0, sgn)):
                field[a, rows_of, :] = value
            return carry

        lax.fori_loop(0, rows // SUB, undo, 0)
        wide = sign_row(rows)
        target = field if forward else out_ref

        def kerr(a, carry):
            x = field[a]
            square = x * x
            magnitude = square + swap(square)
            power = jnp.sum(magnitude, axis=0, keepdims=True)
            sine, cosine = sine_cosine(gain_ref[...] * (2.0 * power - magnitude))
            target[a] = packed_mul(x, cosine, sine * wide)
            return carry

        lax.fori_loop(0, count, kerr, 0, unroll=2)
    if forward:
        source = field if inverse else x_ref

        def apply(c, carry):
            rows_of = chunk(c)
            items = short_fft([source[a, rows_of, :] for a in range(count)], -1.0, sgn)
            for d, value in enumerate(items):
                out_ref[d, rows_of, :] = packed_mul(value, cos_ref[d : d + 1, :], sin_ref[d : d + 1, :])
            return carry

        lax.fori_loop(0, rows // SUB, apply, 0)


def column_stage(x, twist_cos, twist_sin, gain, scale, inverse, forward):
    return pl.pallas_call(
        functools.partial(column_kernel, inverse, forward, scale),
        out_shape=jax.ShapeDtypeStruct(x.shape, x.dtype),
        in_specs=[pl.BlockSpec(memory_space=pltpu.VMEM)] * 4,
        out_specs=pl.BlockSpec(memory_space=pltpu.VMEM),
        scratch_shapes=[pltpu.VMEM(x.shape, jnp.float32)],
        name="column",
    )(x, twist_cos, twist_sin, gain)


def long_dft(x, weights):
    high = x.astype(jnp.bfloat16)
    low = (x - high.astype(jnp.float32)).astype(jnp.bfloat16)
    both = jnp.concatenate((high, low), axis=1)
    product = jnp.dot(both, weights, preferred_element_type=jnp.float32)
    return product[:, :LANES] + product[:, LANES:]


def row_kernel(
    x_ref, c_ref, spread_cos_ref, spread_sin_ref, tw_cos_ref, tw_sin_ref, fwd_ref, inv_ref,
    out_ref, spec, by_real, by_imag, total,
):
    step = pl.program_id(0)
    count, rows = x_ref.shape[0], x_ref.shape[1]
    group, modes, width = c_ref.shape[0], c_ref.shape[1], c_ref.shape[2]
    sgn = sign_row(SUB)
    low = low_lanes((rows, LANES))

    def chunk(c):
        return pl.ds(pl.multiple_of(c * SUB, SUB), SUB)

    @pl.when(step == 0)
    def _():
        total[...] = jnp.zeros_like(total)

        def lanes(q, carry):
            part = pl.ds(q * 4, 4)
            block = x_ref[part].reshape(4 * rows, LANES)
            spec[part] = long_dft(block, fwd_ref[...]).reshape(4, rows, LANES)
            return carry

        lax.fori_loop(0, count // 4, lanes, 0)

        def across(c, carry):
            rows_of = chunk(c)
            items = [
                packed_mul(spec[p, rows_of, :], tw_cos_ref[p : p + 1, :], tw_sin_ref[p : p + 1, :])
                for p in range(count)
            ]
            for j, value in enumerate(short_fft(items, -1.0, sgn)):
                spec[j, rows_of, :] = value
            return carry

        lax.fori_loop(0, rows // SUB, across, 0)

        for tile in range(width // 2):
            first, second = spec[2 * tile], spec[2 * tile + 1]
            real = jnp.where(low, first, swap(second))
            imag = jnp.where(low, swap(first), second)
            for part in range(2):
                by_real[pl.ds(2 * tile + part, rows, stride=width), :] = real
                by_imag[pl.ds(2 * tile + part, rows, stride=width), :] = imag

    odd = lax.broadcasted_iota(jnp.int32, (SUB, LANES), 0) % 2 == 1

    def mix(q, carry):
        with_real = [jnp.zeros((SUB, LANES), jnp.float32) for _ in range(group)]
        with_imag = [jnp.zeros((SUB, LANES), jnp.float32) for _ in range(group)]
        for m in range(modes):
            at = pl.ds(pl.multiple_of(m * width + q * SUB, SUB), SUB)
            real, imag = by_real[at, :], by_imag[at, :]
            for g in range(group):
                factor = c_ref[g, m, chunk(q), :]
                with_real[g] = with_real[g] + factor * real
                with_imag[g] = with_imag[g] + factor * imag
        for g in range(group):
            other = jnp.where(
                odd, pltpu.roll(with_imag[g], 1, 0), -pltpu.roll(with_imag[g], SUB - 1, 0)
            )
            at = pl.ds(pl.multiple_of((step * group + g) * width + q * SUB, SUB), SUB)
            total[at, :] = with_real[g] + other
        return carry

    lax.fori_loop(0, width // SUB, mix, 0)

    @pl.when(step == pl.num_programs(0) - 1)
    def _():
        for tile in range(width // 2):
            first, second = spec[2 * tile], spec[2 * tile + 1]
            at = pl.ds(tile * LANES, LANES)
            real = jnp.where(low, first, swap(second)) + total[pl.ds(2 * tile, rows, stride=width), :]
            imag = jnp.where(low, swap(first), second) + total[
                pl.ds(2 * tile + 1, rows, stride=width), :
            ]
            real, imag = rotate(real, imag, spread_cos_ref[:, at], spread_sin_ref[:, at])
            spec[2 * tile] = jnp.where(low, real, swap(imag))
            spec[2 * tile + 1] = jnp.where(low, swap(real), imag)

        def across(c, carry):
            rows_of = chunk(c)
            items = short_fft([spec[j, rows_of, :] for j in range(count)], 1.0, sgn)
            for p, value in enumerate(items):
                spec[p, rows_of, :] = packed_mul(
                    value, tw_cos_ref[p : p + 1, :], -tw_sin_ref[p : p + 1, :]
                )
            return carry

        lax.fori_loop(0, rows // SUB, across, 0)

        def lanes(q, carry):
            part = pl.ds(q * 4, 4)
            block = spec[part].reshape(4 * rows, LANES)
            out_ref[part] = long_dft(block, inv_ref[...]).reshape(4, rows, LANES)
            return carry

        lax.fori_loop(0, count // 4, lanes, 0)


def row_stage(x, coupling, spread_cos, spread_sin, tw_cos, tw_sin, fwd, inv):
    rows = x.shape[1]
    modes, width = coupling.shape[0], coupling.shape[2]
    group = max(g for g in range(1, 7) if modes % g == 0)
    whole = lambda array: pl.BlockSpec(array.shape, lambda t: (0,) * array.ndim)
    return pl.pallas_call(
        row_kernel,
        grid=(modes // group,),
        out_shape=jax.ShapeDtypeStruct(x.shape, x.dtype),
        in_specs=[
            whole(x),
            pl.BlockSpec((group, modes, width, LANES), lambda t: (t, 0, 0, 0)),
            whole(spread_cos),
            whole(spread_sin),
            whole(tw_cos),
            whole(tw_sin),
            whole(fwd),
            whole(inv),
        ],
        out_specs=whole(x),
        scratch_shapes=[
            pltpu.VMEM(x.shape, jnp.float32),
            pltpu.VMEM((rows * width, LANES), jnp.float32),
            pltpu.VMEM((rows * width, LANES), jnp.float32),
            pltpu.VMEM((rows * width, LANES), jnp.float32),
        ],
        compiler_params=pltpu.CompilerParams(dimension_semantics=("arbitrary",)),
        name="row",
    )(x, coupling, spread_cos, spread_sin, tw_cos, tw_sin, fwd, inv)


def packed_table(cosine, sine):
    xp = np if isinstance(cosine, np.ndarray) else jnp
    return (
        xp.concatenate((cosine, cosine), axis=1).astype(xp.float32),
        xp.concatenate((-sine, sine), axis=1).astype(xp.float32),
    )


def dft_weights(size, orient):
    index = np.arange(size)
    angle = orient * 2.0 * np.pi * (index[:, None] * index[None, :] % size) / size
    cosine, sine = np.cos(angle), np.sin(angle)
    full = np.block([[cosine, sine], [-sine, cosine]]).astype(np.float32)
    high = full.astype(jnp.bfloat16)
    low = (full - high.astype(np.float32)).astype(jnp.bfloat16)
    return np.block([[high, low], [high, np.zeros_like(low)]])


def packed_device(pulses, coupling, dispersion_terms, kerr_gain):
    shards = lax.axis_size("freq")
    device = lax.axis_index("freq")
    modes, local = pulses.shape[2], pulses.shape[3]
    groups = local // shards
    total = local * shards
    rows = -(-modes // SUB) * SUB
    pad = rows - modes

    shard_index = np.arange(shards)
    angle = -2.0 * np.pi * (shard_index[:, None] * np.arange(groups)[None, :] % local) / local
    tw_cos, tw_sin = packed_table(np.cos(angle), np.sin(angle))
    fwd, inv = dft_weights(groups, -1.0), dft_weights(groups, 1.0)
    samples = device + shards * jnp.arange(groups, dtype=jnp.int32)
    twist_cos, twist_sin = packed_table(
        *angle_table(jnp.arange(shards, dtype=jnp.int32), samples, total, -1.0)
    )
    gain = jnp.broadcast_to(jnp.pad(kerr_gain, (0, pad))[:, None], (rows, LANES))

    bins = device + shards * jnp.arange(local, dtype=jnp.int32)
    signed_bin = jnp.where(bins < total // 2, bins, bins - total).astype(jnp.float32)
    angular = signed_bin / (total // 2)
    terms = jnp.pad(dispersion_terms, ((0, 0), (0, pad)))
    dispersion = (
        terms[0][:, None] * angular
        + terms[1][:, None] * angular**2 / 2
        + terms[2][:, None] * angular**3 / 6
    )
    spread_cos, spread_sin = jnp.cos(dispersion), jnp.sin(dispersion)

    coupling = coupling.reshape(2, modes, modes, local // LANES, LANES).transpose(1, 2, 3, 0, 4)
    coupling = coupling.reshape(modes, modes, 2 * local // LANES, LANES)
    blocks = pulses.reshape(2, modes, groups, shards).transpose(3, 1, 0, 2)
    x = jnp.pad(blocks.reshape(shards, modes, 2 * groups), ((0, 0), (0, pad), (0, 0)))
    scale = 1.0 / total
    for repeat in range(STEPS):
        x = exchange(x, modes) if repeat == 0 else x
        if repeat == 0:
            x = column_stage(x, twist_cos, twist_sin, gain, scale, False, True)
        x = exchange(x, modes)
        x = row_stage(x, coupling, spread_cos, spread_sin, tw_cos, tw_sin, fwd, inv)
        x = exchange(x, modes)
        x = column_stage(x, twist_cos, twist_sin, gain, scale, True, repeat < STEPS - 1)
    x = exchange(x, modes)
    x = x[:, :modes].reshape(shards, modes, 2, groups).transpose(2, 1, 3, 0)
    return x.reshape(1, 2, modes, local)


def fits(shards, pulses):
    local = pulses.shape[3] // shards
    return (
        pulses.shape[0] == 1
        and shards & (shards - 1) == 0
        and shards >= 4
        and local == shards * HALF
    )


def solution(mesh):
    in_specs = (P(None, None, None, "freq"), P(None, None, None, "freq"), P(), P())
    out_specs = P(None, None, None, "freq")
    shards = mesh.shape["freq"]

    def run(pulses, coupling, dispersion_terms, kerr_gain):
        body = packed_device if fits(shards, pulses) else per_device
        return jax.shard_map(
            body, mesh=mesh, in_specs=in_specs, out_specs=out_specs, check_vma=False
        )(pulses, coupling, dispersion_terms, kerr_gain)

    return run
```
